64 devices in a mesh: lev: 4 (over x, y), w: 16 (over z, core).
Axes of the slice: x: 2, y: 2, z: 8, core: 2. Of those that a mesh axis runs over, the one named last changes fastest.
The devices are a block of a 4x4x8 slice.
Arguments:
- coef: float32 [320, 2, 192, 320], P('w', None, 'lev'), parts along dimension 2
- legendre: float32 [320, 320, 320], replicated
- gauss_weight: float32 [320], replicated
Outputs:
- output 1: float32 [192, 320, 640], P('lev', 'w'), parts along dimension 0
- output 2: float32 [320, 2, 192, 320], P('w', None, 'lev'), parts along dimension 2
There are 4 independent parts. The reference program is written for one: setup_inputs(seed, part) draws one part's arguments, and reference() takes and returns one part's arrays. A program takes and returns all parts, laid end to end along the dimension named above; an argument that names none is the same for every part.
All inputs are finite; a program needn't handle non-finite values.
Results may differ from the reference program's by a relative error of at most 0.001.
Values sent between devices are 32-bit elements.
A program may use at most 768 MiB of HBM per device.

```python
import jax
import jax.numpy as jnp
from jax import lax

WAVE_NUM = 320
LAT_ROWS = 320
LEVELS = 48


def setup_inputs(seed: int = 0, part: int = 0) -> dict:
    base_key = jax.random.key(seed)
    key_coef = jax.random.fold_in(jax.random.fold_in(base_key, 1), part)
    key_leg = jax.random.fold_in(base_key, 2)
    key_wt = jax.random.fold_in(base_key, 3)
    wave_idx = jnp.arange(WAVE_NUM)
    row_m = wave_idx[:, None].astype(jnp.float32)
    col_l = wave_idx[None, :].astype(jnp.float32)
    live_mask = wave_idx[None, :] >= wave_idx[:, None]
    amplitude = jnp.sqrt(WAVE_NUM / ((WAVE_NUM - row_m) * (1.0 + (col_l - row_m) / WAVE_NUM)))
    coef_mask = jnp.stack([live_mask, live_mask & (wave_idx[:, None] > 0)], axis=1)[:, :, None, :]
    draw_coef = jax.random.normal(key_coef, (WAVE_NUM, 2, LEVELS, WAVE_NUM), jnp.float32)
    coef = jnp.where(coef_mask, draw_coef * amplitude[:, None, None, :], 0.0)
    draw_leg = jax.random.normal(key_leg, (WAVE_NUM, WAVE_NUM, LAT_ROWS), jnp.float32)
    legendre = jnp.where(live_mask[:, :, None], draw_leg, 0.0)
    gauss_weight = jax.random.uniform(key_wt, (LAT_ROWS,), jnp.float32, 0.5, 1.5) / LAT_ROWS
    return {'coef': coef, 'legendre': legendre, 'gauss_weight': gauss_weight}


def reference(coef, legendre, gauss_weight):
    lon_pts = 2 * WAVE_NUM
    splits = 8
    lat_blk = LAT_ROWS // splits

    def lat_step(spec_acc, blk_idx):
        lat_start = blk_idx * lat_blk
        leg_blk = lax.dynamic_slice_in_dim(legendre, lat_start, lat_blk, axis=2).astype(jnp.float32)
        wt_blk = lax.dynamic_slice_in_dim(gauss_weight, lat_start, lat_blk, axis=0)
        fourier = jnp.einsum('mrkl,mlj->mrkj', coef.astype(jnp.float32), leg_blk)
        spec = lax.complex(fourier[:, 0], fourier[:, 1])
        grid_blk = jnp.fft.irfft(spec, n=lon_pts, axis=0)
        square_hat = jnp.fft.rfft(grid_blk * grid_blk, axis=0)[:WAVE_NUM] * wt_blk[None, None, :]
        re_im = jnp.stack([jnp.real(square_hat), jnp.imag(square_hat)], axis=1)
        spec_acc = spec_acc + jnp.einsum('mrkj,mlj->mrkl', re_im, leg_blk)
        return spec_acc, jnp.transpose(grid_blk, (1, 2, 0))

    spec_out, grid_parts = lax.scan(lat_step, jnp.zeros(coef.shape, jnp.float32), jnp.arange(splits))
    grid = jnp.transpose(grid_parts, (1, 0, 2, 3)).reshape(LEVELS, LAT_ROWS, lon_pts)
    return grid, spec_out
```

```python
import functools

import jax
import jax.numpy as jnp
import numpy as np
from jax import lax
from jax.experimental import pallas as pl
from jax.experimental.pallas import tpu as pltpu
from jax.sharding import PartitionSpec as P

MESH = pl.DeviceIdType.MESH
F32, BF16 = jnp.float32, jnp.bfloat16

RUN_START = (0, 8, 16)
RUN_LEN = (8, 8, 4)
LEV = 16
JPACK = 4


def split(x):
    hi = x.astype(BF16)
    return hi, (x - hi.astype(F32)).astype(BF16)


def dot3(a, b, dims):
    (ah, al), (bh, bl) = a, b
    mul = functools.partial(lax.dot_general, dimension_numbers=(dims, ((), ())), preferred_element_type=F32)
    return mul(ah, bh) + mul(al, bh) + mul(ah, bl)


def fourier_matrix(wave_num, group, wave_loc):
    lon = 2 * wave_num
    slots = []
    for start, length in zip(RUN_START, RUN_LEN):
        for dev in range(group):
            slots += [dev * wave_loc + start + i for i in range(length)]
    pad = -len(slots) % 128
    wave = np.array(slots)
    phase = (np.arange(lon)[:, None] * wave[None, :]) % lon
    ang = 2.0 * np.pi * phase / lon
    blank = np.zeros((lon, pad))
    full = np.concatenate([np.cos(ang), blank, -np.sin(ang), blank], axis=1).astype(np.float32)
    hi = full.astype(jnp.bfloat16)
    lo = (full - hi.astype(np.float32)).astype(jnp.bfloat16)
    return hi, lo


def kernel(group, coef_hbm, leg_hbm, wt_ref, ehi_hbm, elo_hbm, grid_hbm, out_hbm,
           coef, leg, leg_hi, leg_lo, ehi, elo,
           ft, wa, wb, w4, wc, ra, rb, rc, xc, lhs, qhi, qlo, ha, hb, hc, sa, sb, sc, s4, bmat, grid, spec,
           load_sem, const_sem, send1, recv1, send2, recv2, grid_sem, out_sem):
    me = lax.axis_index('w')
    wave_loc, lat = coef.shape[0], leg.shape[1]
    lat_loc = lat // group
    chunks = coef.shape[2] // LEV
    lon = ehi.shape[0]
    jgs = lat_loc // JPACK
    rows80 = group * jgs
    lane = lax.broadcasted_iota(jnp.int32, (rows80, 128), 1)

    barrier = pltpu.get_barrier_semaphore()

    def greet(i, carry):
        pl.semaphore_signal(barrier, inc=1, device_id={'w': lax.rem(me + i, group)}, device_id_type=MESH)
        return carry
    lax.fori_loop(1, group, greet, 0)

    def load(m):
        a = pltpu.make_async_copy(coef_hbm.at[m], coef.at[m], load_sem.at[0, m])
        b = pltpu.make_async_copy(leg_hbm.at[me * wave_loc + m], leg.at[m], load_sem.at[1, m])
        return a, b

    def start_load(m, carry):
        a, b = load(m)
        a.start()
        b.start()
        return carry
    lax.fori_loop(0, wave_loc, start_load, 0)
    load_e = [pltpu.make_async_copy(ehi_hbm, ehi, const_sem.at[0]), pltpu.make_async_copy(elo_hbm, elo, const_sem.at[1])]
    for cp in load_e:
        cp.start()

    xc[...] = jnp.zeros_like(xc)

    def pieces(bufs, c, dev, run):
        buf = bufs[run]
        if run < 2:
            return buf.at[c, pl.ds(pl.multiple_of(dev * (8 * jgs), 8), 8 * jgs), :]
        return buf.at[c, dev]

    def send(src, dst, ssem, rsem, c, run):
        def one(i, carry):
            to = lax.rem(me + i, group)
            pltpu.make_async_remote_copy(
                pieces(src, c, to, run), pieces(dst, c, me, run), ssem.at[c, run], rsem.at[c, run],
                device_id={'w': to}, device_id_type=MESH).start()
            return carry
        lax.fori_loop(1, group, one, 0)
        if run < 2:
            at = pl.ds(pl.multiple_of(me * (8 * jgs), 8), 8 * jgs)
            dst[run][c, at, :] = src[run][c, at, :]
        else:
            dst[run][c, me] = src[run][c, me]

    def all_bytes(bufs, c, run):
        if run < 2:
            return bufs[run].at[c, pl.ds(0, (group - 1) * 8 * jgs), :]
        return bufs[run].at[c, pl.ds(0, group - 1)]

    def wait(bufs, sem, c, run):
        ref = all_bytes(bufs, c, run)
        pltpu.make_async_copy(ref, ref, sem.at[c, run]).wait()

    src1, dst1 = (wa, wb, wc), (ra, rb, rc)
    src2, dst2 = (ha, hb, hc), (sa, sb, sc)

    def inverse(m, mm, run):
        a, b = load(m)
        a.wait()
        b.wait()
        lh, ll = split(leg[m])
        leg_hi[m] = lh
        leg_lo[m] = ll
        scale = jnp.where(me * wave_loc + m == 0, 1.0 / lon, 2.0 / lon).astype(F32)
        f = dot3(split(coef[m].reshape(2 * chunks * LEV, lat)), (lh, ll), ((1,), (0,))) * scale
        ft[:, 0:2 * chunks * LEV] = f.T
        vals = [None] * chunks
        for jj in range(JPACK):
            x = ft[pl.ds(jj, rows80, stride=JPACK), :]
            rolled = {}
            for c in range(chunks):
                for r in range(2):
                    s = (LEV * ((JPACK - chunks) * r + jj - c)) % 128
                    if s not in rolled:
                        rolled[s] = x if s == 0 else pltpu.roll(x, s, 1)
                    to = r * 64 + jj * LEV
                    mask = (lane >= to) & (lane < to + LEV)
                    vals[c] = rolled[s] if vals[c] is None else jnp.where(mask, rolled[s], vals[c])
        for c in range(chunks):
            if run < 2:
                (wa, wb)[run][c, pl.ds(mm, rows80, stride=8), :] = vals[c]
            else:
                w4[c, pl.ds(mm, rows80, stride=4), :] = vals[c]

    for run in range(3):
        def body(mm, carry, run=run):
            inverse(RUN_START[run] + mm, mm, run)
            return carry
        lax.fori_loop(0, RUN_LEN[run], body, 0)
        if run == 2:
            for c in range(chunks):
                for d in range(group):
                    wc[c, d] = w4[c, 4 * jgs * d:4 * jgs * (d + 1), :]
        if run == 0:
            pl.semaphore_wait(barrier, group - 1)
        send(src1, dst1, send1, recv1, 0, run)
    for c in range(1, chunks):
        for run in range(3):
            send(src1, dst1, send1, recv1, c, run)
    for cp in load_e:
        cp.wait()

    def latitudes(c, carry):
        for run in range(3):
            wait(dst1, recv1, c, run)
        for jg in range(jgs):
            for s in range(group):
                xc[jg, 4 * s:4 * s + 4, :] = rc[c, s, 4 * jg:4 * jg + 4, :]
        rows = JPACK * LEV
        for jg in range(jgs):
            for run in range(3):
                if run < 2:
                    buf = (ra, rb)[run]
                    x = jnp.concatenate([buf[c, 8 * (jgs * s + jg):8 * (jgs * s + jg) + 8, :] for s in range(group)], axis=0)
                else:
                    x = xc[jg]
                xt = x.T
                lhs[rows * jg:rows * (jg + 1), 128 * run:128 * (run + 1)] = xt[:rows]
                lhs[rows * jg:rows * (jg + 1), 384 + 128 * run:384 + 128 * (run + 1)] = xt[rows:]
        e = (ehi[...], elo[...])
        g = dot3(split(lhs[...]), e, ((1,), (1,)))
        for j in range(lat_loc):
            gj = g[LEV * j:LEV * (j + 1), :]
            grid[pl.ds(c * LEV, LEV), j, :] = gj
            q = gj * gj * wt_ref[me * lat_loc + j]
            hi, lo = split(q)
            qhi[LEV * j:LEV * (j + 1), :] = hi
            qlo[LEV * j:LEV * (j + 1), :] = lo
        lhs[...] = dot3((qhi[...], qlo[...]), e, ((1,), (0,)))
        for jg in range(jgs):
            for run in range(3):
                a = lhs[rows * jg:rows * (jg + 1), 128 * run:128 * (run + 1)]
                b = lhs[rows * jg:rows * (jg + 1), 384 + 128 * run:384 + 128 * (run + 1)]
                h = jnp.concatenate([a, b], axis=0).T
                for s in range(group):
                    if run < 2:
                        (ha, hb)[run][c, 8 * (jgs * s + jg):8 * (jgs * s + jg) + 8, :] = h[8 * s:8 * s + 8]
                    else:
                        hc[c, s, 4 * jg:4 * jg + 4, :] = h[4 * s:4 * s + 4]
        for run in range(3):
            send(src2, dst2, send2, recv2, c, run)
        at = pl.ds(pl.multiple_of(c * LEV, LEV), LEV)
        pltpu.make_async_copy(grid.at[at], grid_hbm.at[at], grid_sem.at[c]).start()
        return carry
    lax.fori_loop(0, chunks, latitudes, 0)

    def forward(c, run, m0, mm0, src, stride):
        for mi in range(4):
            y = src[c, pl.ds(mm0 + mi, rows80, stride=stride), :] if stride == 8 else src[pl.ds(mm0 + mi, rows80, stride=stride), :]
            for jj in range(JPACK):
                s0 = (32 * mi - LEV * jj) % 128
                s1 = (32 * mi - 48 - LEV * jj) % 128
                y0 = y if s0 == 0 else pltpu.roll(y, s0, 1)
                y1 = y if s1 == 0 else pltpu.roll(y, s1, 1)
                to = 32 * mi
                v = jnp.where((lane >= to) & (lane < to + 16), y0, jnp.where((lane >= to + 16) & (lane < to + 32), y1, 0.0))
                bmat[mi, pl.ds(jj, rows80, stride=JPACK), :] = v
        acc = None
        for mi in range(4):
            t = dot3((leg_hi[m0 + mi], leg_lo[m0 + mi]), split(bmat[mi]), ((1,), (0,)))
            acc = t if acc is None else acc + t
        o = acc.T
        for mi in range(4):
            for r in range(2):
                spec[m0 + mi, r, pl.ds(pl.multiple_of(c * LEV, LEV), LEV), :] = o[32 * mi + 16 * r:32 * mi + 16 * (r + 1)]

    def out_copy(c, run):
        ms = pl.ds(RUN_START[run], RUN_LEN[run])
        at = pl.ds(pl.multiple_of(c * LEV, LEV), LEV)
        return pltpu.make_async_copy(spec.at[ms, :, at, :], out_hbm.at[ms, :, at, :], out_sem.at[c, run])

    def spectral(c, carry):
        for run in range(3):
            wait(dst2, recv2, c, run)
            if run < 2:
                def half(i, carry2, run=run):
                    forward(c, run, RUN_START[run] + 4 * i, 4 * i, (sa, sb)[run], 8)
                    return carry2
                lax.fori_loop(0, 2, half, 0)
            else:
                for s in range(group):
                    s4[4 * jgs * s:4 * jgs * (s + 1), :] = sc[c, s]
                forward(c, run, RUN_START[2], 0, s4, 4)
            out_copy(c, run).start()
        return carry
    lax.fori_loop(0, chunks, spectral, 0)

    def drain(c, carry):
        for run in range(3):
            wait(src1, send1, c, run)
            wait(src2, send2, c, run)
            out_copy(c, run).wait()
        at = pl.ds(pl.multiple_of(c * LEV, LEV), LEV)
        pltpu.make_async_copy(grid.at[at], grid_hbm.at[at], grid_sem.at[c]).wait()
        return carry
    lax.fori_loop(0, chunks, drain, 0)


def solution(mesh):
    group = mesh.shape['w']

    def per_device(coef, legendre, gauss_weight):
        wave_loc, _, levels, degrees = coef.shape
        lat = legendre.shape[2]
        lat_loc = lat // group
        wave_num = wave_loc * group
        lon = 2 * wave_num
        chunks = levels // LEV
        jgs = lat_loc // JPACK
        ehi, elo = fourier_matrix(wave_num, group, wave_loc)
        cols = ehi.shape[1]
        big = (chunks, group * jgs * 8, 128)
        small = (chunks, group, 4 * jgs, 128)
        vm = pltpu.VMEM
        any_spec = pl.BlockSpec(memory_space=pl.ANY)
        return pl.pallas_call(
            functools.partial(kernel, group),
            out_shape=(jax.ShapeDtypeStruct((levels, lat_loc, lon), F32), jax.ShapeDtypeStruct(coef.shape, F32)),
            in_specs=[any_spec, any_spec, pl.BlockSpec(memory_space=pltpu.SMEM), any_spec, any_spec],
            out_specs=(any_spec, any_spec),
            scratch_shapes=[
                vm(coef.shape, F32), vm((wave_loc, degrees, lat), F32),
                vm((wave_loc, degrees, lat), BF16), vm((wave_loc, degrees, lat), BF16),
                vm((lon, cols), BF16), vm((lon, cols), BF16),
                vm((lat, 128), F32),
                vm(big, F32), vm(big, F32), vm((chunks, group * jgs * 4, 128), F32), vm(small, F32),
                vm(big, F32), vm(big, F32), vm(small, F32),
                vm((jgs, 128, 128), F32), vm((lat_loc * LEV, cols), F32),
                vm((lat_loc * LEV, lon), BF16), vm((lat_loc * LEV, lon), BF16),
                vm(big, F32), vm(big, F32), vm(small, F32),
                vm(big, F32), vm(big, F32), vm(small, F32), vm((group * jgs * 4, 128), F32),
                vm((4, lat, 128), F32),
                vm((levels, lat_loc, lon), F32), vm(coef.shape, F32),
                pltpu.SemaphoreType.DMA((2, wave_loc)), pltpu.SemaphoreType.DMA((2,)),
                pltpu.SemaphoreType.DMA((chunks, 3)), pltpu.SemaphoreType.DMA((chunks, 3)),
                pltpu.SemaphoreType.DMA((chunks, 3)), pltpu.SemaphoreType.DMA((chunks, 3)),
                pltpu.SemaphoreType.DMA((chunks,)), pltpu.SemaphoreType.DMA((chunks, 3)),
            ],
            compiler_params=pltpu.CompilerParams(
                collective_id=0, has_side_effects=True, vmem_limit_bytes=62 * 1024 * 1024),
        )(coef, legendre, gauss_weight, jnp.asarray(ehi), jnp.asarray(elo))

    return jax.shard_map(
        per_device, mesh=mesh,
        in_specs=(P('w', None, 'lev', None), P(None, None, None), P(None)),
        out_specs=(P('lev', 'w', None), P('w', None, 'lev', None)), check_vma=False)
```

```python
import functools

import jax
import jax.numpy as jnp
import numpy as np
from jax import lax
from jax.experimental import pallas as pl
from jax.experimental.pallas import tpu as pltpu
from jax.sharding import PartitionSpec as P

MESH = pl.DeviceIdType.MESH
F32, BF16 = jnp.float32, jnp.bfloat16

RUN_START = (0, 8, 16)
RUN_LEN = (8, 8, 4)
LEV = 16
JPACK = 4


def split(x):
    hi = x.astype(BF16)
    return hi, (x - hi.astype(F32)).astype(BF16)


def product(a, b, dims):
    return lax.dot_general(a, b, dimension_numbers=(dims, ((), ())), preferred_element_type=F32)


def dot3_rows(a, b, dims):
    (ah, al), (bh, bl) = a, b
    both = product(jnp.concatenate([ah, al], axis=0), bh, dims)
    n = ah.shape[0]
    return both[:n] + both[n:] + product(ah, bl, dims)


def dot3_lanes(a, b):
    (ah, al), (bh, bl) = a, b
    both = product(ah, jnp.concatenate([bh, bl], axis=1), ((1,), (0,)))
    return both[:, :128] + both[:, 128:] + product(al, bh, ((1,), (0,)))


def fourier_matrix(wave_num, group, wave_loc):
    lon = 2 * wave_num
    slots = []
    for start, length in zip(RUN_START, RUN_LEN):
        for dev in range(group):
            slots += [dev * wave_loc + start + i for i in range(length)]
    pad = -len(slots) % 128
    wave = np.array(slots)
    phase = (np.arange(lon)[:, None] * wave[None, :]) % lon
    ang = 2.0 * np.pi * phase / lon
    blank = np.zeros((lon, pad))
    full = np.concatenate([np.cos(ang), blank, -np.sin(ang), blank], axis=1).astype(np.float32)
    hi = full.astype(jnp.bfloat16)
    lo = (full - hi.astype(np.float32)).astype(jnp.bfloat16)
    return hi, lo


def forward_tile(rows, table, bmat):
    acc = None
    for mi in range(4):
        y = rows(mi)
        lane = lax.broadcasted_iota(jnp.int32, y.shape, 1)
        to = 32 * mi
        for jj in range(JPACK):
            s0 = (to - LEV * jj) % 128
            s1 = (to - 48 - LEV * jj) % 128
            y0 = y if s0 == 0 else pltpu.roll(y, s0, 1)
            y1 = y if s1 == 0 else pltpu.roll(y, s1, 1)
            v = jnp.where((lane >= to) & (lane < to + 16), y0, jnp.where((lane >= to + 16) & (lane < to + 32), y1, 0.0))
            bmat[mi, pl.ds(jj, y.shape[0], stride=JPACK), :] = v
        t = dot3_lanes(table(mi), split(bmat[mi]))
        acc = t if acc is None else acc + t
    return acc.T


def kernel(group, coef_hbm, leg_hbm, wt_ref, ehi_hbm, elo_hbm, grid, spec, s4, tail_hi, tail_lo,
           coef, leg, leg_hi, leg_lo, ehi, elo,
           ft0, ft1, wa, wb, w4, wc, ra, rb, rc, xc, lhs, qhi, qlo, ha, hb, hc, sa, sb, sc, bmat,
           load_sem, const_sem, send1, recv1, send2, recv2):
    me = lax.axis_index('w')
    wave_loc, lat = coef.shape[0], leg.shape[1]
    lat_loc = lat // group
    chunks = coef.shape[2] // LEV
    lon = ehi.shape[0]
    jgs = lat_loc // JPACK
    rows80 = group * jgs
    lane = lax.broadcasted_iota(jnp.int32, (rows80, 128), 1)

    barrier = pltpu.get_barrier_semaphore()

    def greet(i, carry):
        pl.semaphore_signal(barrier, inc=1, device_id={'w': lax.rem(me + i, group)}, device_id_type=MESH)
        return carry
    lax.fori_loop(1, group, greet, 0)

    def load(m):
        a = pltpu.make_async_copy(coef_hbm.at[m], coef.at[m], load_sem.at[0, m])
        b = pltpu.make_async_copy(leg_hbm.at[me * wave_loc + m], leg.at[m], load_sem.at[1, m])
        return a, b

    def order(i):
        return lax.rem(i + RUN_START[2], wave_loc)

    def start_load(i):
        for cp in load(order(i)):
            cp.start()

    for i in range(RUN_LEN[2]):
        start_load(i)
    load_e = [pltpu.make_async_copy(ehi_hbm, ehi, const_sem.at[0]), pltpu.make_async_copy(elo_hbm, elo, const_sem.at[1])]
    xc[...] = jnp.zeros_like(xc)

    def pieces(bufs, c, dev, run):
        buf = bufs[run]
        if run < 2:
            return buf.at[c, pl.ds(pl.multiple_of(dev * (8 * jgs), 8), 8 * jgs), :]
        return buf.at[c, dev]

    def send(src, dst, ssem, rsem, c, run):
        def one(j, carry):
            i = group - j
            to = lax.rem(me + group + (2 * lax.rem(i, 2) - 1) * ((i + 1) // 2), group)
            pltpu.make_async_remote_copy(
                pieces(src, c, to, run), pieces(dst, c, me, run), ssem.at[c, run], rsem.at[c, run],
                device_id={'w': to}, device_id_type=MESH).start()
            return carry
        lax.fori_loop(1, group, one, 0)
        if run < 2:
            at = pl.ds(pl.multiple_of(me * (8 * jgs), 8), 8 * jgs)
            dst[run][c, at, :] = src[run][c, at, :]
        else:
            dst[run][c, me] = src[run][c, me]

    def all_bytes(bufs, c, run):
        if run < 2:
            return bufs[run].at[c, pl.ds(0, (group - 1) * 8 * jgs), :]
        return bufs[run].at[c, pl.ds(0, group - 1)]

    def wait(bufs, sem, c, run):
        ref = all_bytes(bufs, c, run)
        pltpu.make_async_copy(ref, ref, sem.at[c, run]).wait()

    src1, dst1 = (wa, wb, wc), (ra, rb, rc)
    src2, dst2 = (ha, hb, hc), (sa, sb, sc)

    def inverse(m, mm, run, ft):
        lh, ll = split(leg[m])
        if run < 2:
            leg_hi[m] = lh
            leg_lo[m] = ll
        else:
            tail_hi[mm] = lh
            tail_lo[mm] = ll
        scale = jnp.where(me * wave_loc + m == 0, 1.0 / lon, 2.0 / lon).astype(F32)
        f = dot3_rows(split(coef[m].reshape(2 * chunks * LEV, lat)), (lh, ll), ((1,), (0,))) * scale
        ft[:, 0:2 * chunks * LEV] = f.T
        vals = [None] * chunks
        for jj in range(JPACK):
            x = ft[pl.ds(jj, rows80, stride=JPACK), :]
            rolled = {}
            for c in range(chunks):
                for r in range(2):
                    s = (LEV * ((JPACK - chunks) * r + jj - c)) % 128
                    if s not in rolled:
                        rolled[s] = x if s == 0 else pltpu.roll(x, s, 1)
                    to = r * 64 + jj * LEV
                    mask = (lane >= to) & (lane < to + LEV)
                    vals[c] = rolled[s] if vals[c] is None else jnp.where(mask, rolled[s], vals[c])
        for c in range(chunks):
            if run < 2:
                (wa, wb)[run][c, pl.ds(mm, rows80, stride=8), :] = vals[c]
            else:
                w4[c, pl.ds(mm, rows80, stride=4), :] = vals[c]

    done = 0
    for run in (2, 0, 1):
        def pair(i, carry, run=run, done=done):
            for k in range(2):
                @pl.when(done + 2 * i + k + RUN_LEN[2] < wave_loc)
                def _(k=k):
                    start_load(done + 2 * i + k + RUN_LEN[2])
            for k in range(2):
                for cp in load(RUN_START[run] + 2 * i + k):
                    cp.wait()
            for k, ft in ((0, ft0), (1, ft1)):
                inverse(RUN_START[run] + 2 * i + k, 2 * i + k, run, ft)
            return carry
        lax.fori_loop(0, RUN_LEN[run] // 2, pair, 0)
        done += RUN_LEN[run]
        if run == 2:
            for cp in load_e:
                cp.start()
            for c in range(chunks):
                for d in range(group):
                    wc[c, d] = w4[c, 4 * jgs * d:4 * jgs * (d + 1), :]
            pl.semaphore_wait(barrier, group - 1)
            for c in range(chunks):
                send(src1, dst1, send1, recv1, c, run)
        else:
            send(src1, dst1, send1, recv1, 0, run)
    for c in range(1, chunks):
        for run in range(2):
            send(src1, dst1, send1, recv1, c, run)
    for cp in load_e:
        cp.wait()

    def latitudes(c, carry):
        for run in range(3):
            wait(dst1, recv1, c, run)
        for jg in range(jgs):
            for s in range(group):
                xc[jg, 4 * s:4 * s + 4, :] = rc[c, s, 4 * jg:4 * jg + 4, :]
        rows = JPACK * LEV
        for jg in range(jgs):
            for run in range(3):
                if run < 2:
                    buf = (ra, rb)[run]
                    x = jnp.concatenate([buf[c, 8 * (jgs * s + jg):8 * (jgs * s + jg) + 8, :] for s in range(group)], axis=0)
                else:
                    x = xc[jg]
                xt = x.T
                lhs[rows * jg:rows * (jg + 1), 128 * run:128 * (run + 1)] = xt[:rows]
                lhs[rows * jg:rows * (jg + 1), 384 + 128 * run:384 + 128 * (run + 1)] = xt[rows:]
        e = (ehi[...], elo[...])
        g = dot3_rows(split(lhs[...]), e, ((1,), (1,)))
        for j in range(lat_loc):
            gj = g[LEV * j:LEV * (j + 1), :]
            grid[j, pl.ds(pl.multiple_of(c * LEV, LEV), LEV), :] = gj
            q = gj * gj * wt_ref[me * lat_loc + j]
            hi, lo = split(q)
            qhi[LEV * j:LEV * (j + 1), :] = hi
            qlo[LEV * j:LEV * (j + 1), :] = lo
        lhs[...] = dot3_rows((qhi[...], qlo[...]), e, ((1,), (0,)))
        for jg in range(jgs):
            for run in range(3):
                a = lhs[rows * jg:rows * (jg + 1), 128 * run:128 * (run + 1)]
                b = lhs[rows * jg:rows * (jg + 1), 384 + 128 * run:384 + 128 * (run + 1)]
                h = jnp.concatenate([a, b], axis=0).T
                for s in range(group):
                    if run < 2:
                        (ha, hb)[run][c, 8 * (jgs * s + jg):8 * (jgs * s + jg) + 8, :] = h[8 * s:8 * s + 8]
                    else:
                        hc[c, s, 4 * jg:4 * jg + 4, :] = h[4 * s:4 * s + 4]
        for run in range(3):
            send(src2, dst2, send2, recv2, c, run)
        return carry
    lax.fori_loop(0, chunks, latitudes, 0)

    def forward(c, run, mm0):
        m0 = RUN_START[run] + mm0
        if run < 2:
            rows = lambda mi: (sa, sb)[run][c, pl.ds(mm0 + mi, rows80, stride=8), :]
            table = lambda mi: (leg_hi[m0 + mi], leg_lo[m0 + mi])
        else:
            rows = lambda mi: s4[pl.ds(mi, rows80, stride=4), :]
            table = lambda mi: (tail_hi[mi], tail_lo[mi])
        o = forward_tile(rows, table, bmat)
        for mi in range(4):
            for r in range(2):
                spec[m0 + mi, r, pl.ds(pl.multiple_of(c * LEV, LEV), LEV), :] = o[32 * mi + 16 * r:32 * mi + 16 * (r + 1)]

    def spectral(c, carry):
        for run in range(3):
            wait(dst2, recv2, c, run)
            if run < 2:
                def half(i, carry2, run=run):
                    forward(c, run, 4 * i)
                    return carry2
                lax.fori_loop(0, 2, half, 0)
            else:
                for s in range(group):
                    s4[4 * jgs * s:4 * jgs * (s + 1), :] = sc[c, s]

                @pl.when(c < chunks - 1)
                def _():
                    forward(c, 2, 0)
        return carry
    lax.fori_loop(0, chunks, spectral, 0)

    def drain(c, carry):
        for run in range(3):
            wait(src1, send1, c, run)
            wait(src2, send2, c, run)
        return carry
    lax.fori_loop(0, chunks, drain, 0)


def write_out(grid, spec, last, tail_hi, tail_lo, grid_hbm, spec_hbm, bmat, piece, sem):
    half = grid.shape[0] // 2
    m0, left = RUN_START[2], spec.shape[2] - LEV
    piece_hbm = spec_hbm.at[pl.ds(m0, RUN_LEN[2]), :, pl.ds(left, LEV), :]
    copies = [
        pltpu.make_async_copy(grid.at[pl.ds(0, half)], grid_hbm.at[pl.ds(0, half)], sem.at[0]),
        pltpu.make_async_copy(grid.at[pl.ds(half, half)], grid_hbm.at[pl.ds(half, half)], sem.at[1]),
        pltpu.make_async_copy(spec.at[pl.ds(0, m0 // 2)], spec_hbm.at[pl.ds(0, m0 // 2)], sem.at[2]),
        pltpu.make_async_copy(spec.at[pl.ds(m0 // 2, m0 // 2)], spec_hbm.at[pl.ds(m0 // 2, m0 // 2)], sem.at[3]),
        pltpu.make_async_copy(spec.at[pl.ds(m0, RUN_LEN[2]), :, pl.ds(0, left), :],
                              spec_hbm.at[pl.ds(m0, RUN_LEN[2]), :, pl.ds(0, left), :], sem.at[4]),
    ]
    for cp in copies:
        cp.start()
    rows80 = last.shape[0] // 4
    o = forward_tile(lambda mi: last[pl.ds(mi, rows80, stride=4), :], lambda mi: (tail_hi[mi], tail_lo[mi]), bmat)
    for mi in range(RUN_LEN[2]):
        for r in range(2):
            piece[mi, r] = o[32 * mi + 16 * r:32 * mi + 16 * (r + 1)]
    cp = pltpu.make_async_copy(piece, piece_hbm, sem.at[5])
    cp.start()
    for cp in copies + [cp]:
        cp.wait()


def solution(mesh):
    group = mesh.shape['w']

    def per_device(coef, legendre, gauss_weight):
        wave_loc, _, levels, degrees = coef.shape
        lat = legendre.shape[2]
        lat_loc = lat // group
        wave_num = wave_loc * group
        lon = 2 * wave_num
        chunks = levels // LEV
        jgs = lat_loc // JPACK
        ehi, elo = fourier_matrix(wave_num, group, wave_loc)
        cols = ehi.shape[1]
        big = (chunks, group * jgs * 8, 128)
        small = (chunks, group, 4 * jgs, 128)
        vm = pltpu.VMEM
        any_spec = pl.BlockSpec(memory_space=pl.ANY)
        grid, spec, last, tail_hi, tail_lo = pl.pallas_call(
            functools.partial(kernel, group),
            out_shape=(vm((lat_loc, levels, lon), F32), vm(coef.shape, F32), vm((group * jgs * 4, 128), F32),
                       vm((RUN_LEN[2], degrees, lat), BF16), vm((RUN_LEN[2], degrees, lat), BF16)),
            in_specs=[any_spec, any_spec, pl.BlockSpec(memory_space=pltpu.SMEM), any_spec, any_spec],
            out_specs=(pl.BlockSpec(memory_space=vm),) * 5,
            scratch_shapes=[
                vm(coef.shape, F32), vm((wave_loc, degrees, lat), F32),
                vm((RUN_START[2], degrees, lat), BF16), vm((RUN_START[2], degrees, lat), BF16),
                vm((lon, cols), BF16), vm((lon, cols), BF16),
                vm((lat, 128), F32), vm((lat, 128), F32),
                vm(big, F32), vm(big, F32), vm((chunks, group * jgs * 4, 128), F32), vm(small, F32),
                vm(big, F32), vm(big, F32), vm(small, F32),
                vm((jgs, 128, 128), F32), vm((lat_loc * LEV, cols), F32),
                vm((lat_loc * LEV, lon), BF16), vm((lat_loc * LEV, lon), BF16),
                vm(big, F32), vm(big, F32), vm(small, F32),
                vm(big, F32), vm(big, F32), vm(small, F32),
                vm((4, lat, 128), F32),
                pltpu.SemaphoreType.DMA((2, wave_loc)), pltpu.SemaphoreType.DMA((2,)),
                pltpu.SemaphoreType.DMA((chunks, 3)), pltpu.SemaphoreType.DMA((chunks, 3)),
                pltpu.SemaphoreType.DMA((chunks, 3)), pltpu.SemaphoreType.DMA((chunks, 3)),
            ],
            compiler_params=pltpu.CompilerParams(
                collective_id=0, has_side_effects=True, vmem_limit_bytes=50 * 1024 * 1024),
        )(coef, legendre, gauss_weight, jnp.asarray(ehi), jnp.asarray(elo))
        grid, spec = pl.pallas_call(
            write_out,
            out_shape=(jax.ShapeDtypeStruct(grid.shape, F32), jax.ShapeDtypeStruct(spec.shape, F32)),
            in_specs=[any_spec, any_spec, pl.BlockSpec(memory_space=vm), pl.BlockSpec(memory_space=vm), pl.BlockSpec(memory_space=vm)],
            out_specs=(pl.BlockSpec(memory_space=pltpu.HBM), pl.BlockSpec(memory_space=pltpu.HBM)),
            scratch_shapes=[vm((4, lat, 128), F32), vm((RUN_LEN[2], 2, LEV, degrees), F32), pltpu.SemaphoreType.DMA((6,))],
            compiler_params=pltpu.CompilerParams(vmem_limit_bytes=12 * 1024 * 1024),
        )(grid, spec, last, tail_hi, tail_lo)
        return jnp.transpose(grid, (1, 0, 2)), spec

    return jax.shard_map(
        per_device, mesh=mesh,
        in_specs=(P('w', None, 'lev', None), P(None, None, None), P(None)),
        out_specs=(P('lev', 'w', None), P('w', None, 'lev', None)), check_vma=False)
```

```python
import functools

import jax
import jax.numpy as jnp
import numpy as np
from jax import lax
from jax.experimental import pallas as pl
from jax.experimental.pallas import tpu as pltpu
from jax.sharding import PartitionSpec as P

MESH = pl.DeviceIdType.MESH
F32, BF16 = jnp.float32, jnp.bfloat16

RUN_START = (0, 8, 16)
RUN_LEN = (8, 8, 4)
LEV = 16
JPACK = 4


def split(x):
    hi = x.astype(BF16)
    return hi, (x - hi.astype(F32)).astype(BF16)


def product(a, b, dims):
    return lax.dot_general(a, b, dimension_numbers=(dims, ((), ())), preferred_element_type=F32)


def dot3_rows(a, b, dims):
    (ah, al), (bh, bl) = a, b
    both = product(jnp.concatenate([ah, al], axis=0), bh, dims)
    n = ah.shape[0]
    return both[:n] + both[n:] + product(ah, bl, dims)


def dot3_lanes(a, b):
    (ah, al), (bh, bl) = a, b
    both = product(ah, jnp.concatenate([bh, bl], axis=1), ((1,), (0,)))
    return both[:, :128] + both[:, 128:] + product(al, bh, ((1,), (0,)))


def fourier_matrix(wave_num, group, wave_loc):
    lon = 2 * wave_num
    slots = []
    for start, length in zip(RUN_START, RUN_LEN):
        for dev in range(group):
            slots += [dev * wave_loc + start + i for i in range(length)]
    pad = -len(slots) % 128
    wave = np.array(slots)
    phase = (np.arange(lon)[:, None] * wave[None, :]) % lon
    ang = 2.0 * np.pi * phase / lon
    blank = np.zeros((lon, pad))
    full = np.concatenate([np.cos(ang), blank, -np.sin(ang), blank], axis=1).astype(np.float32)
    hi = full.astype(jnp.bfloat16)
    lo = (full - hi.astype(np.float32)).astype(jnp.bfloat16)
    return hi, lo


def forward_tile(rows, table, bmat):
    acc = None
    for mi in range(4):
        y = rows(mi)
        lane = lax.broadcasted_iota(jnp.int32, y.shape, 1)
        to = 32 * mi
        for jj in range(JPACK):
            s0 = (to - LEV * jj) % 128
            s1 = (to - 48 - LEV * jj) % 128
            y0 = y if s0 == 0 else pltpu.roll(y, s0, 1)
            y1 = y if s1 == 0 else pltpu.roll(y, s1, 1)
            v = jnp.where((lane >= to) & (lane < to + 16), y0, jnp.where((lane >= to + 16) & (lane < to + 32), y1, 0.0))
            bmat[mi, pl.ds(jj, y.shape[0], stride=JPACK), :] = v
        t = dot3_lanes(table(mi), split(bmat[mi]))
        acc = t if acc is None else acc + t
    return acc.T


def kernel(group, coef_hbm, leg_hbm, wt_hbm, ehi_hbm, elo_hbm, grid, spec, s4, tail_hi, tail_lo,
           coef, leg, leg_hi, leg_lo, ehi, elo,
           ft0, ft1, wa, wb, w4, wc, ra, rb, rc, xc, lhs, qhi, qlo, ha, hb, hc, sa, sb, sc, bmat,
           wt, load_sem, const_sem, send1, recv1, send2, recv2):
    me = lax.axis_index('w')
    wave_loc, lat = coef.shape[0], leg.shape[1]
    lat_loc = lat // group
    chunks = coef.shape[2] // LEV
    lon = ehi.shape[0]
    jgs = lat_loc // JPACK
    rows80 = group * jgs
    lane = lax.broadcasted_iota(jnp.int32, (rows80, 128), 1)

    barrier = pltpu.get_barrier_semaphore()

    def peer(i):
        far = group - i
        return lax.rem(me + group + (2 * lax.rem(far, 2) - 1) * ((far + 1) // 2), group)

    for i in range(1, group):
        pl.semaphore_signal(barrier, inc=1, device_id={'w': peer(i)}, device_id_type=MESH)

    def load(m):
        a = pltpu.make_async_copy(coef_hbm.at[m], coef.at[m], load_sem.at[0, m])
        b = pltpu.make_async_copy(leg_hbm.at[me * wave_loc + m], leg.at[m], load_sem.at[1, m])
        return a, b

    def order(i):
        return lax.rem(i + RUN_START[2], wave_loc)

    def start_load(i):
        for cp in load(order(i)):
            cp.start()

    for i in range(RUN_LEN[2]):
        start_load(i)
    load_e = [pltpu.make_async_copy(ehi_hbm, ehi, const_sem.at[0]), pltpu.make_async_copy(elo_hbm, elo, const_sem.at[1]),
              pltpu.make_async_copy(wt_hbm, wt, const_sem.at[2])]
    xc[...] = jnp.zeros_like(xc)

    ring = group // 2
    peers = [p for d in range(1, ring // 2) for p in ((d, 0), (-d, 1), (-d, 0), (d, 1))]
    peers += [(ring // 2, 0), (ring // 2, 1), (0, 1)]

    def pieces(bufs, c, dev, run):
        buf = bufs[run]
        if run < 2:
            return buf.at[c, pl.ds(pl.multiple_of(dev * (8 * jgs), 8), 8 * jgs), :]
        return buf.at[c, dev]

    def send(src, dst, ssem, rsem, c, run):
        for dist, core in peers:
            to = lax.rem(me // 2 + dist + ring, ring) * 2 + lax.rem(me + core, 2)
            pltpu.make_async_remote_copy(
                pieces(src, c, to, run), pieces(dst, c, me, run), ssem.at[c, run], rsem.at[c, run],
                device_id={'w': to}, device_id_type=MESH).start()
        if run < 2:
            at = pl.ds(pl.multiple_of(me * (8 * jgs), 8), 8 * jgs)
            dst[run][c, at, :] = src[run][c, at, :]
        else:
            dst[run][c, me] = src[run][c, me]

    def all_bytes(bufs, c, run):
        if run < 2:
            return bufs[run].at[c, pl.ds(0, (group - 1) * 8 * jgs), :]
        return bufs[run].at[c, pl.ds(0, group - 1)]

    def wait(bufs, sem, c, run):
        ref = all_bytes(bufs, c, run)
        pltpu.make_async_copy(ref, ref, sem.at[c, run]).wait()

    src1, dst1 = (wa, wb, wc), (ra, rb, rc)
    src2, dst2 = (ha, hb, hc), (sa, sb, sc)

    def inverse(m, mm, run, ft):
        lh, ll = split(leg[m])
        if run < 2:
            leg_hi[m] = lh
            leg_lo[m] = ll
        else:
            tail_hi[mm] = lh
            tail_lo[mm] = ll
        scale = jnp.where(me * wave_loc + m == 0, 1.0 / lon, 2.0 / lon).astype(F32)
        f = dot3_rows(split(coef[m].reshape(2 * chunks * LEV, lat)), (lh, ll), ((1,), (0,))) * scale
        ft[:, 0:2 * chunks * LEV] = f.T
        vals = [None] * chunks
        for jj in range(JPACK):
            x = ft[pl.ds(jj, rows80, stride=JPACK), :]
            rolled = {}
            for c in range(chunks):
                for r in range(2):
                    s = (LEV * ((JPACK - chunks) * r + jj - c)) % 128
                    if s not in rolled:
                        rolled[s] = x if s == 0 else pltpu.roll(x, s, 1)
                    to = r * 64 + jj * LEV
                    mask = (lane >= to) & (lane < to + LEV)
                    vals[c] = rolled[s] if vals[c] is None else jnp.where(mask, rolled[s], vals[c])
        for c in range(chunks):
            if run < 2:
                (wa, wb)[run][c, pl.ds(mm, rows80, stride=8), :] = vals[c]
            else:
                w4[c, pl.ds(mm, rows80, stride=4), :] = vals[c]

    done = 0
    for run in (2, 0, 1):
        def pair(i, carry, run=run, done=done):
            for k in range(2):
                @pl.when(done + 2 * i + k + RUN_LEN[2] < wave_loc)
                def _(k=k):
                    start_load(done + 2 * i + k + RUN_LEN[2])
            for k in range(2):
                for cp in load(RUN_START[run] + 2 * i + k):
                    cp.wait()
            for k, ft in ((0, ft0), (1, ft1)):
                inverse(RUN_START[run] + 2 * i + k, 2 * i + k, run, ft)
            return carry
        lax.fori_loop(0, RUN_LEN[run] // 2, pair, 0)
        done += RUN_LEN[run]
        if run == 2:
            for cp in load_e:
                cp.start()
            for c in range(chunks):
                for d in range(group):
                    wc[c, d] = w4[c, 4 * jgs * d:4 * jgs * (d + 1), :]
            pl.semaphore_wait(barrier, group - 1)
            for c in range(chunks):
                send(src1, dst1, send1, recv1, c, run)
        else:
            send(src1, dst1, send1, recv1, 0, run)
    for c in range(1, chunks):
        for run in range(2):
            send(src1, dst1, send1, recv1, c, run)
    for cp in load_e:
        cp.wait()

    def latitudes(c, carry):
        for run in range(3):
            wait(dst1, recv1, c, run)
        for jg in range(jgs):
            for s in range(group):
                xc[jg, 4 * s:4 * s + 4, :] = rc[c, s, 4 * jg:4 * jg + 4, :]
        rows = JPACK * LEV
        for jg in range(jgs):
            for run in range(3):
                if run < 2:
                    buf = (ra, rb)[run]
                    x = jnp.concatenate([buf[c, 8 * (jgs * s + jg):8 * (jgs * s + jg) + 8, :] for s in range(group)], axis=0)
                else:
                    x = xc[jg]
                xt = x.T
                lhs[rows * jg:rows * (jg + 1), 128 * run:128 * (run + 1)] = xt[:rows]
                lhs[rows * jg:rows * (jg + 1), 384 + 128 * run:384 + 128 * (run + 1)] = xt[rows:]
        e = (ehi[...], elo[...])
        g = dot3_rows(split(lhs[...]), e, ((1,), (1,)))
        for j in range(lat_loc):
            gj = g[LEV * j:LEV * (j + 1), :]
            grid[j, pl.ds(pl.multiple_of(c * LEV, LEV), LEV), :] = gj
            q = gj * gj * wt[me * lat_loc + j]
            hi, lo = split(q)
            qhi[LEV * j:LEV * (j + 1), :] = hi
            qlo[LEV * j:LEV * (j + 1), :] = lo
        lhs[...] = dot3_rows((qhi[...], qlo[...]), e, ((1,), (0,)))
        for jg in range(jgs):
            for run in range(3):
                a = lhs[rows * jg:rows * (jg + 1), 128 * run:128 * (run + 1)]
                b = lhs[rows * jg:rows * (jg + 1), 384 + 128 * run:384 + 128 * (run + 1)]
                h = jnp.concatenate([a, b], axis=0).T
                for s in range(group):
                    if run < 2:
                        (ha, hb)[run][c, 8 * (jgs * s + jg):8 * (jgs * s + jg) + 8, :] = h[8 * s:8 * s + 8]
                    else:
                        hc[c, s, 4 * jg:4 * jg + 4, :] = h[4 * s:4 * s + 4]
        for run in range(3):
            send(src2, dst2, send2, recv2, c, run)
        return carry
    lax.fori_loop(0, chunks, latitudes, 0)

    def forward(c, run, mm0):
        m0 = RUN_START[run] + mm0
        if run < 2:
            rows = lambda mi: (sa, sb)[run][c, pl.ds(mm0 + mi, rows80, stride=8), :]
            table = lambda mi: (leg_hi[m0 + mi], leg_lo[m0 + mi])
        else:
            rows = lambda mi: s4[pl.ds(mi, rows80, stride=4), :]
            table = lambda mi: (tail_hi[mi], tail_lo[mi])
        o = forward_tile(rows, table, bmat)
        for mi in range(4):
            for r in range(2):
                spec[m0 + mi, r, pl.ds(pl.multiple_of(c * LEV, LEV), LEV), :] = o[32 * mi + 16 * r:32 * mi + 16 * (r + 1)]

    def spectral(c, carry):
        for run in range(3):
            wait(dst2, recv2, c, run)
            if run < 2:
                def half(i, carry2, run=run):
                    forward(c, run, 4 * i)
                    return carry2
                lax.fori_loop(0, 2, half, 0)
            else:
                for s in range(group):
                    s4[4 * jgs * s:4 * jgs * (s + 1), :] = sc[c, s]

                @pl.when(c < chunks - 1)
                def _():
                    forward(c, 2, 0)
        return carry
    lax.fori_loop(0, chunks, spectral, 0)

    def drain(c, carry):
        for run in range(3):
            wait(src1, send1, c, run)
            wait(src2, send2, c, run)
        return carry
    lax.fori_loop(0, chunks, drain, 0)


def write_out(grid, spec, last, tail_hi, tail_lo, grid_hbm, spec_hbm, bmat, piece, sem):
    half = grid.shape[0] // 2
    m0, left = RUN_START[2], spec.shape[2] - LEV
    piece_hbm = spec_hbm.at[pl.ds(m0, RUN_LEN[2]), :, pl.ds(left, LEV), :]
    copies = [
        pltpu.make_async_copy(grid.at[pl.ds(0, half)], grid_hbm.at[pl.ds(0, half)], sem.at[0]),
        pltpu.make_async_copy(grid.at[pl.ds(half, half)], grid_hbm.at[pl.ds(half, half)], sem.at[1]),
        pltpu.make_async_copy(spec.at[pl.ds(0, m0 // 2)], spec_hbm.at[pl.ds(0, m0 // 2)], sem.at[2]),
        pltpu.make_async_copy(spec.at[pl.ds(m0 // 2, m0 // 2)], spec_hbm.at[pl.ds(m0 // 2, m0 // 2)], sem.at[3]),
        pltpu.make_async_copy(spec.at[pl.ds(m0, RUN_LEN[2]), :, pl.ds(0, left), :],
                              spec_hbm.at[pl.ds(m0, RUN_LEN[2]), :, pl.ds(0, left), :], sem.at[4]),
    ]
    for cp in copies:
        cp.start()
    rows80 = last.shape[0] // 4
    o = forward_tile(lambda mi: last[pl.ds(mi, rows80, stride=4), :], lambda mi: (tail_hi[mi], tail_lo[mi]), bmat)
    for mi in range(RUN_LEN[2]):
        for r in range(2):
            piece[mi, r] = o[32 * mi + 16 * r:32 * mi + 16 * (r + 1)]
    cp = pltpu.make_async_copy(piece, piece_hbm, sem.at[5])
    cp.start()
    for cp in copies + [cp]:
        cp.wait()


def solution(mesh):
    group = mesh.shape['w']

    def per_device(coef, legendre, gauss_weight):
        wave_loc, _, levels, degrees = coef.shape
        lat = legendre.shape[2]
        lat_loc = lat // group
        wave_num = wave_loc * group
        lon = 2 * wave_num
        chunks = levels // LEV
        jgs = lat_loc // JPACK
        ehi, elo = fourier_matrix(wave_num, group, wave_loc)
        cols = ehi.shape[1]
        big = (chunks, group * jgs * 8, 128)
        small = (chunks, group, 4 * jgs, 128)
        vm = pltpu.VMEM
        any_spec = pl.BlockSpec(memory_space=pl.ANY)
        grid, spec, last, tail_hi, tail_lo = pl.pallas_call(
            functools.partial(kernel, group),
            out_shape=(vm((lat_loc, levels, lon), F32), vm(coef.shape, F32), vm((group * jgs * 4, 128), F32),
                       vm((RUN_LEN[2], degrees, lat), BF16), vm((RUN_LEN[2], degrees, lat), BF16)),
            in_specs=[any_spec] * 5,
            out_specs=(pl.BlockSpec(memory_space=vm),) * 5,
            scratch_shapes=[
                vm(coef.shape, F32), vm((wave_loc, degrees, lat), F32),
                vm((RUN_START[2], degrees, lat), BF16), vm((RUN_START[2], degrees, lat), BF16),
                vm((lon, cols), BF16), vm((lon, cols), BF16),
                vm((lat, 128), F32), vm((lat, 128), F32),
                vm(big, F32), vm(big, F32), vm((chunks, group * jgs * 4, 128), F32), vm(small, F32),
                vm(big, F32), vm(big, F32), vm(small, F32),
                vm((jgs, 128, 128), F32), vm((lat_loc * LEV, cols), F32),
                vm((lat_loc * LEV, lon), BF16), vm((lat_loc * LEV, lon), BF16),
                vm(big, F32), vm(big, F32), vm(small, F32),
                vm(big, F32), vm(big, F32), vm(small, F32),
                vm((4, lat, 128), F32),
                pltpu.SMEM((lat,), F32), pltpu.SemaphoreType.DMA((2, wave_loc)), pltpu.SemaphoreType.DMA((3,)),
                pltpu.SemaphoreType.DMA((chunks, 3)), pltpu.SemaphoreType.DMA((chunks, 3)),
                pltpu.SemaphoreType.DMA((chunks, 3)), pltpu.SemaphoreType.DMA((chunks, 3)),
            ],
            compiler_params=pltpu.CompilerParams(
                collective_id=0, has_side_effects=True, vmem_limit_bytes=50 * 1024 * 1024),
        )(coef, legendre, gauss_weight, jnp.asarray(ehi), jnp.asarray(elo))
        grid, spec = pl.pallas_call(
            write_out,
            out_shape=(jax.ShapeDtypeStruct(grid.shape, F32), jax.ShapeDtypeStruct(spec.shape, F32)),
            in_specs=[any_spec, any_spec, pl.BlockSpec(memory_space=vm), pl.BlockSpec(memory_space=vm), pl.BlockSpec(memory_space=vm)],
            out_specs=(pl.BlockSpec(memory_space=pltpu.HBM), pl.BlockSpec(memory_space=pltpu.HBM)),
            scratch_shapes=[vm((4, lat, 128), F32), vm((RUN_LEN[2], 2, LEV, degrees), F32), pltpu.SemaphoreType.DMA((6,))],
            compiler_params=pltpu.CompilerParams(vmem_limit_bytes=12 * 1024 * 1024),
        )(grid, spec, last, tail_hi, tail_lo)
        return jnp.transpose(grid, (1, 0, 2)), spec

    return jax.shard_map(
        per_device, mesh=mesh,
        in_specs=(P('w', None, 'lev', None), P(None, None, None), P(None)),
        out_specs=(P('lev', 'w', None), P('w', None, 'lev', None)), check_vma=False)
```

```python
import functools

import jax
import jax.numpy as jnp
import numpy as np
from jax import lax
from jax.experimental import pallas as pl
from jax.experimental.pallas import tpu as pltpu
from jax.sharding import PartitionSpec as P

MESH = pl.DeviceIdType.MESH
F32, BF16 = jnp.float32, jnp.bfloat16

RUN_START = (0, 8, 16)
RUN_LEN = (8, 8, 4)
LEV = 16
JPACK = 4


def split(x):
    hi = x.astype(BF16)
    return hi, (x - hi.astype(F32)).astype(BF16)


def product(a, b, dims):
    return lax.dot_general(a, b, dimension_numbers=(dims, ((), ())), preferred_element_type=F32)


def dot3_rows(a, b, dims):
    (ah, al), (bh, bl) = a, b
    both = product(jnp.concatenate([ah, al], axis=0), bh, dims)
    n = ah.shape[0]
    return both[:n] + both[n:] + product(ah, bl, dims)


def dot3_lanes(a, b):
    (ah, al), (bh, bl) = a, b
    both = product(ah, jnp.concatenate([bh, bl], axis=1), ((1,), (0,)))
    return both[:, :128] + both[:, 128:] + product(al, bh, ((1,), (0,)))


def fourier_matrix(wave_num, group, wave_loc):
    lon = 2 * wave_num
    slots = []
    for start, length in zip(RUN_START, RUN_LEN):
        for dev in range(group):
            slots += [dev * wave_loc + start + i for i in range(length)]
    pad = -len(slots) % 128
    wave = np.array(slots)
    phase = (np.arange(lon)[:, None] * wave[None, :]) % lon
    ang = 2.0 * np.pi * phase / lon
    blank = np.zeros((lon, pad))
    full = np.concatenate([np.cos(ang), blank, -np.sin(ang), blank], axis=1).astype(np.float32)
    hi = full.astype(jnp.bfloat16)
    lo = (full - hi.astype(np.float32)).astype(jnp.bfloat16)
    return hi, lo


def forward_tile(rows, table, bmat):
    acc = None
    for mi in range(4):
        y = rows(mi)
        lane = lax.broadcasted_iota(jnp.int32, y.shape, 1)
        to = 32 * mi
        for jj in range(JPACK):
            s0 = (to - LEV * jj) % 128
            s1 = (to - 48 - LEV * jj) % 128
            y0 = y if s0 == 0 else pltpu.roll(y, s0, 1)
            y1 = y if s1 == 0 else pltpu.roll(y, s1, 1)
            v = jnp.where((lane >= to) & (lane < to + 16), y0, jnp.where((lane >= to + 16) & (lane < to + 32), y1, 0.0))
            bmat[mi, pl.ds(jj, y.shape[0], stride=JPACK), :] = v
        t = dot3_lanes(table(mi), split(bmat[mi]))
        acc = t if acc is None else acc + t
    return acc.T


def kernel(group, coef_hbm, leg_hbm, wt_hbm, ehi_hbm, elo_hbm, grid, spec, s4, tail_hi, tail_lo,
           coef, leg, leg_hi, leg_lo, ehi, elo,
           ft0, ft1, wa, wb, w4, wc, ra, rb, rc, xc, lhs, qhi, qlo, ha, hb, hc, sa, sb, sc, bmat,
           wt, load_sem, const_sem, send1, recv1, send2, recv2):
    me = lax.axis_index('w')
    wave_loc, lat = coef.shape[0], leg.shape[1]
    lat_loc = lat // group
    chunks = coef.shape[2] // LEV
    lon = ehi.shape[0]
    jgs = lat_loc // JPACK
    rows80 = group * jgs
    lane = lax.broadcasted_iota(jnp.int32, (rows80, 128), 1)

    barrier = pltpu.get_barrier_semaphore()

    def peer(i):
        far = group - i
        return lax.rem(me + group + (2 * lax.rem(far, 2) - 1) * ((far + 1) // 2), group)

    for i in range(1, group):
        pl.semaphore_signal(barrier, inc=1, device_id={'w': peer(i)}, device_id_type=MESH)

    def load(m):
        a = pltpu.make_async_copy(coef_hbm.at[m], coef.at[m], load_sem.at[0, m])
        b = pltpu.make_async_copy(leg_hbm.at[me * wave_loc + m], leg.at[m], load_sem.at[1, m])
        return a, b

    def order(i):
        return lax.rem(i + RUN_START[2], wave_loc)

    def start_load(i):
        for cp in load(order(i)):
            cp.start()

    for i in range(RUN_LEN[2]):
        start_load(i)
    load_e = [pltpu.make_async_copy(ehi_hbm, ehi, const_sem.at[0]), pltpu.make_async_copy(elo_hbm, elo, const_sem.at[1]),
              pltpu.make_async_copy(wt_hbm, wt, const_sem.at[2])]
    xc[...] = jnp.zeros_like(xc)

    ring = group // 2
    peers = [p for d in range(1, ring // 2) for p in ((d, 0), (-d, 1), (-d, 0), (d, 1))]
    peers = [(0, 1)] + peers + [(ring // 2, 0), (ring // 2, 1)]

    def pieces(bufs, c, dev, run):
        buf = bufs[run]
        if run < 2:
            return buf.at[c, pl.ds(pl.multiple_of(dev * (8 * jgs), 8), 8 * jgs), :]
        return buf.at[c, dev]

    def send(src, dst, ssem, rsem, c, run):
        for dist, core in peers:
            to = lax.rem(me // 2 + dist + ring, ring) * 2 + lax.rem(me + core, 2)
            pltpu.make_async_remote_copy(
                pieces(src, c, to, run), pieces(dst, c, me, run), ssem.at[c, run], rsem.at[c, run],
                device_id={'w': to}, device_id_type=MESH).start()
        if run < 2:
            at = pl.ds(pl.multiple_of(me * (8 * jgs), 8), 8 * jgs)
            dst[run][c, at, :] = src[run][c, at, :]
        else:
            dst[run][c, me] = src[run][c, me]

    def all_bytes(bufs, c, run):
        if run < 2:
            return bufs[run].at[c, pl.ds(0, (group - 1) * 8 * jgs), :]
        return bufs[run].at[c, pl.ds(0, group - 1)]

    def wait(bufs, sem, c, run):
        ref = all_bytes(bufs, c, run)
        pltpu.make_async_copy(ref, ref, sem.at[c, run]).wait()

    src1, dst1 = (wa, wb, wc), (ra, rb, rc)
    src2, dst2 = (ha, hb, hc), (sa, sb, sc)

    def inverse(m, mm, run, ft):
        lh, ll = split(leg[m])
        if run < 2:
            leg_hi[m] = lh
            leg_lo[m] = ll
        else:
            tail_hi[mm] = lh
            tail_lo[mm] = ll
        scale = jnp.where(me * wave_loc + m == 0, 1.0 / lon, 2.0 / lon).astype(F32)
        f = dot3_rows(split(coef[m].reshape(2 * chunks * LEV, lat)), (lh, ll), ((1,), (0,))) * scale
        ft[:, 0:2 * chunks * LEV] = f.T
        vals = [None] * chunks
        for jj in range(JPACK):
            x = ft[pl.ds(jj, rows80, stride=JPACK), :]
            rolled = {}
            for c in range(chunks):
                for r in range(2):
                    s = (LEV * ((JPACK - chunks) * r + jj - c)) % 128
                    if s not in rolled:
                        rolled[s] = x if s == 0 else pltpu.roll(x, s, 1)
                    to = r * 64 + jj * LEV
                    mask = (lane >= to) & (lane < to + LEV)
                    vals[c] = rolled[s] if vals[c] is None else jnp.where(mask, rolled[s], vals[c])
        for c in range(chunks):
            if run < 2:
                (wa, wb)[run][c, pl.ds(mm, rows80, stride=8), :] = vals[c]
            else:
                w4[c, pl.ds(mm, rows80, stride=4), :] = vals[c]

    done = 0
    for run in (2, 0, 1):
        def pair(i, carry, run=run, done=done):
            for k in range(2):
                @pl.when(done + 2 * i + k + RUN_LEN[2] < wave_loc)
                def _(k=k):
                    start_load(done + 2 * i + k + RUN_LEN[2])
            for k in range(2):
                for cp in load(RUN_START[run] + 2 * i + k):
                    cp.wait()
            for k, ft in ((0, ft0), (1, ft1)):
                inverse(RUN_START[run] + 2 * i + k, 2 * i + k, run, ft)
            return carry
        lax.fori_loop(0, RUN_LEN[run] // 2, pair, 0)
        done += RUN_LEN[run]
        if run == 2:
            for cp in load_e:
                cp.start()
            for c in range(chunks):
                for d in range(group):
                    wc[c, d] = w4[c, 4 * jgs * d:4 * jgs * (d + 1), :]
            pl.semaphore_wait(barrier, group - 1)
            for c in range(chunks):
                send(src1, dst1, send1, recv1, c, run)
        else:
            send(src1, dst1, send1, recv1, 0, run)
    for c in range(1, chunks):
        for run in range(2):
            send(src1, dst1, send1, recv1, c, run)
    for cp in load_e:
        cp.wait()

    def latitudes(c, carry):
        for run in range(3):
            wait(dst1, recv1, c, run)
        for jg in range(jgs):
            for s in range(group):
                xc[jg, 4 * s:4 * s + 4, :] = rc[c, s, 4 * jg:4 * jg + 4, :]
        rows = JPACK * LEV
        for jg in range(jgs):
            for run in range(3):
                if run < 2:
                    buf = (ra, rb)[run]
                    x = jnp.concatenate([buf[c, 8 * (jgs * s + jg):8 * (jgs * s + jg) + 8, :] for s in range(group)], axis=0)
                else:
                    x = xc[jg]
                xt = x.T
                lhs[rows * jg:rows * (jg + 1), 128 * run:128 * (run + 1)] = xt[:rows]
                lhs[rows * jg:rows * (jg + 1), 384 + 128 * run:384 + 128 * (run + 1)] = xt[rows:]
        e = (ehi[...], elo[...])
        g = dot3_rows(split(lhs[...]), e, ((1,), (1,)))
        for j in range(lat_loc):
            gj = g[LEV * j:LEV * (j + 1), :]
            grid[j, pl.ds(pl.multiple_of(c * LEV, LEV), LEV), :] = gj
            q = gj * gj * wt[me * lat_loc + j]
            hi, lo = split(q)
            qhi[LEV * j:LEV * (j + 1), :] = hi
            qlo[LEV * j:LEV * (j + 1), :] = lo
        lhs[...] = dot3_rows((qhi[...], qlo[...]), e, ((1,), (0,)))
        for jg in range(jgs):
            for run in range(3):
                a = lhs[rows * jg:rows * (jg + 1), 128 * run:128 * (run + 1)]
                b = lhs[rows * jg:rows * (jg + 1), 384 + 128 * run:384 + 128 * (run + 1)]
                h = jnp.concatenate([a, b], axis=0).T
                for s in range(group):
                    if run < 2:
                        (ha, hb)[run][c, 8 * (jgs * s + jg):8 * (jgs * s + jg) + 8, :] = h[8 * s:8 * s + 8]
                    else:
                        hc[c, s, 4 * jg:4 * jg + 4, :] = h[4 * s:4 * s + 4]
        for run in range(3):
            send(src2, dst2, send2, recv2, c, run)
        return carry
    lax.fori_loop(0, chunks, latitudes, 0)

    def forward(c, run, mm0):
        m0 = RUN_START[run] + mm0
        if run < 2:
            rows = lambda mi: (sa, sb)[run][c, pl.ds(mm0 + mi, rows80, stride=8), :]
            table = lambda mi: (leg_hi[m0 + mi], leg_lo[m0 + mi])
        else:
            rows = lambda mi: s4[pl.ds(mi, rows80, stride=4), :]
            table = lambda mi: (tail_hi[mi], tail_lo[mi])
        o = forward_tile(rows, table, bmat)
        for mi in range(4):
            for r in range(2):
                spec[m0 + mi, r, pl.ds(pl.multiple_of(c * LEV, LEV), LEV), :] = o[32 * mi + 16 * r:32 * mi + 16 * (r + 1)]

    def spectral(c, carry):
        for run in range(3):
            wait(dst2, recv2, c, run)
            if run < 2:
                def half(i, carry2, run=run):
                    forward(c, run, 4 * i)
                    return carry2
                lax.fori_loop(0, 2, half, 0)
            else:
                for s in range(group):
                    s4[4 * jgs * s:4 * jgs * (s + 1), :] = sc[c, s]

                @pl.when(c < chunks - 1)
                def _():
                    forward(c, 2, 0)
        return carry
    lax.fori_loop(0, chunks, spectral, 0)

    def drain(c, carry):
        for run in range(3):
            wait(src1, send1, c, run)
            wait(src2, send2, c, run)
        return carry
    lax.fori_loop(0, chunks, drain, 0)


def write_out(grid, spec, last, tail_hi, tail_lo, grid_hbm, spec_hbm, bmat, piece, sem):
    half = grid.shape[0] // 2
    m0, left = RUN_START[2], spec.shape[2] - LEV
    piece_hbm = spec_hbm.at[pl.ds(m0, RUN_LEN[2]), :, pl.ds(left, LEV), :]
    copies = [
        pltpu.make_async_copy(grid.at[pl.ds(0, half)], grid_hbm.at[pl.ds(0, half)], sem.at[0]),
        pltpu.make_async_copy(grid.at[pl.ds(half, half)], grid_hbm.at[pl.ds(half, half)], sem.at[1]),
        pltpu.make_async_copy(spec.at[pl.ds(0, m0 // 2)], spec_hbm.at[pl.ds(0, m0 // 2)], sem.at[2]),
        pltpu.make_async_copy(spec.at[pl.ds(m0 // 2, m0 // 2)], spec_hbm.at[pl.ds(m0 // 2, m0 // 2)], sem.at[3]),
        pltpu.make_async_copy(spec.at[pl.ds(m0, RUN_LEN[2]), :, pl.ds(0, left), :],
                              spec_hbm.at[pl.ds(m0, RUN_LEN[2]), :, pl.ds(0, left), :], sem.at[4]),
    ]
    for cp in copies:
        cp.start()
    rows80 = last.shape[0] // 4
    o = forward_tile(lambda mi: last[pl.ds(mi, rows80, stride=4), :], lambda mi: (tail_hi[mi], tail_lo[mi]), bmat)
    for mi in range(RUN_LEN[2]):
        for r in range(2):
            piece[mi, r] = o[32 * mi + 16 * r:32 * mi + 16 * (r + 1)]
    cp = pltpu.make_async_copy(piece, piece_hbm, sem.at[5])
    cp.start()
    for cp in copies + [cp]:
        cp.wait()


def solution(mesh):
    group = mesh.shape['w']

    def per_device(coef, legendre, gauss_weight):
        wave_loc, _, levels, degrees = coef.shape
        lat = legendre.shape[2]
        lat_loc = lat // group
        wave_num = wave_loc * group
        lon = 2 * wave_num
        chunks = levels // LEV
        jgs = lat_loc // JPACK
        ehi, elo = fourier_matrix(wave_num, group, wave_loc)
        cols = ehi.shape[1]
        big = (chunks, group * jgs * 8, 128)
        small = (chunks, group, 4 * jgs, 128)
        vm = pltpu.VMEM
        any_spec = pl.BlockSpec(memory_space=pl.ANY)
        grid, spec, last, tail_hi, tail_lo = pl.pallas_call(
            functools.partial(kernel, group),
            out_shape=(vm((lat_loc, levels, lon), F32), vm(coef.shape, F32), vm((group * jgs * 4, 128), F32),
                       vm((RUN_LEN[2], degrees, lat), BF16), vm((RUN_LEN[2], degrees, lat), BF16)),
            in_specs=[any_spec] * 5,
            out_specs=(pl.BlockSpec(memory_space=vm),) * 5,
            scratch_shapes=[
                vm(coef.shape, F32), vm((wave_loc, degrees, lat), F32),
                vm((RUN_START[2], degrees, lat), BF16), vm((RUN_START[2], degrees, lat), BF16),
                vm((lon, cols), BF16), vm((lon, cols), BF16),
                vm((lat, 128), F32), vm((lat, 128), F32),
                vm(big, F32), vm(big, F32), vm((chunks, group * jgs * 4, 128), F32), vm(small, F32),
                vm(big, F32), vm(big, F32), vm(small, F32),
                vm((jgs, 128, 128), F32), vm((lat_loc * LEV, cols), F32),
                vm((lat_loc * LEV, lon), BF16), vm((lat_loc * LEV, lon), BF16),
                vm(big, F32), vm(big, F32), vm(small, F32),
                vm(big, F32), vm(big, F32), vm(small, F32),
                vm((4, lat, 128), F32),
                pltpu.SMEM((lat,), F32), pltpu.SemaphoreType.DMA((2, wave_loc)), pltpu.SemaphoreType.DMA((3,)),
                pltpu.SemaphoreType.DMA((chunks, 3)), pltpu.SemaphoreType.DMA((chunks, 3)),
                pltpu.SemaphoreType.DMA((chunks, 3)), pltpu.SemaphoreType.DMA((chunks, 3)),
            ],
            compiler_params=pltpu.CompilerParams(
                collective_id=0, has_side_effects=True, vmem_limit_bytes=50 * 1024 * 1024),
        )(coef, legendre, gauss_weight, jnp.asarray(ehi), jnp.asarray(elo))
        grid, spec = pl.pallas_call(
            write_out,
            out_shape=(jax.ShapeDtypeStruct(grid.shape, F32), jax.ShapeDtypeStruct(spec.shape, F32)),
            in_specs=[any_spec, any_spec, pl.BlockSpec(memory_space=vm), pl.BlockSpec(memory_space=vm), pl.BlockSpec(memory_space=vm)],
            out_specs=(pl.BlockSpec(memory_space=pltpu.HBM), pl.BlockSpec(memory_space=pltpu.HBM)),
            scratch_shapes=[vm((4, lat, 128), F32), vm((RUN_LEN[2], 2, LEV, degrees), F32), pltpu.SemaphoreType.DMA((6,))],
            compiler_params=pltpu.CompilerParams(vmem_limit_bytes=12 * 1024 * 1024),
        )(grid, spec, last, tail_hi, tail_lo)
        return jnp.transpose(grid, (1, 0, 2)), spec

    return jax.shard_map(
        per_device, mesh=mesh,
        in_specs=(P('w', None, 'lev', None), P(None, None, None), P(None)),
        out_specs=(P('lev', 'w', None), P('w', None, 'lev', None)), check_vma=False)
```
